8 devices in a mesh: tg: 2 (over z, y), pp: 2 (over x), grp: 2 (over core).
Axes of the slice: x: 2, y: 2, z: 1, core: 2. Of those that a mesh axis runs over, the one named last changes fastest.
Arguments:
- hidden_in: bfloat16 [256, 2048], P(('pp', 'grp'))
- seq_lens: int32 [256], P(('pp', 'grp'))
- k_cache: bfloat16 [2, 256, 128, 16, 128], P(None, ('pp', 'grp'), None, 'tg')
- v_cache: bfloat16 [2, 256, 128, 16, 128], P(None, ('pp', 'grp'), None, 'tg')
- attn_gain: bfloat16 [2, 2048], P('pp')
- w_qkv: bfloat16 [2, 6144, 2048], P('pp', ('tg', 'grp'))
- w_o: bfloat16 [2, 2048, 2048], P('pp', None, ('tg', 'grp'))
- mlp_gain: bfloat16 [2, 2048], P('pp')
- w_gate_up: bfloat16 [2, 11008, 2048], P('pp', ('tg', 'grp'))
- w_down: bfloat16 [2, 2048, 5504], P('pp', None, ('tg', 'grp'))
Outputs:
- output 1: bfloat16 [256, 2048], P(('pp', 'grp'))
- output 2: bfloat16 [2, 256, 128, 16, 128], P(None, ('pp', 'grp'), None, 'tg')
- output 3: bfloat16 [2, 256, 128, 16, 128], P(None, ('pp', 'grp'), None, 'tg')
- output 4: bfloat16 [2, 6144, 2048], P(None, 'tg')
- output 5: bfloat16 [2, 11008, 2048], P(None, 'tg')
All inputs are finite; a program needn't handle non-finite values.
Results may differ from the reference program's by a relative error of at most 0.0121501.
Values are sent between devices in bfloat16 or wider.
A program may use at most 1 GiB of HBM per device.

```python
import jax
import jax.numpy as jnp
from jax import lax
import math

MODEL_DIM = 2048
FFN_DIM = 5504
HEADS = 16
KV_HEADS = 16
HEAD_DIM = 128
LAYERS = 2
GEN_TP = 2
TRAIN_TP = 4
BATCH = 256
CACHE_LEN = 128

ROPE_THETA = 500000.0
NORM_EPS = 1e-5
MASK_FILL = -1e30


def draw_lens(key):
    key_len, key_top = jax.random.split(key)
    drawn = jax.random.randint(key_len, (BATCH,), CACHE_LEN // 8, CACHE_LEN)
    top_row = jax.random.randint(key_top, (), 0, BATCH)
    return jnp.where(jnp.arange(BATCH) == top_row, CACHE_LEN - 1, drawn).astype(jnp.int32)


def setup_inputs(seed: int = 0) -> dict:
    key_list = jax.random.split(jax.random.key(seed), 11)
    qkv_rows = (HEADS + 2 * KV_HEADS) * HEAD_DIM
    cache_shape = (LAYERS, BATCH, CACHE_LEN, KV_HEADS, HEAD_DIM)
    key_scale = math.sqrt(0.5 * math.log(CACHE_LEN))
    hidden_in = jax.random.normal(key_list[0], (BATCH, MODEL_DIM), jnp.float32)
    seq_lens = draw_lens(key_list[1])
    k_cache = jax.random.normal(key_list[2], cache_shape, jnp.float32) * key_scale
    v_mean = jax.random.normal(key_list[3], (LAYERS, BATCH, 1, KV_HEADS, HEAD_DIM), jnp.float32)
    v_cache = 0.5 * v_mean + jax.random.normal(key_list[4], cache_shape, jnp.float32)
    attn_gain = jax.random.uniform(key_list[5], (LAYERS, MODEL_DIM), jnp.float32, 0.2, 1.8)
    w_qkv = jax.random.normal(key_list[6], (LAYERS, qkv_rows, MODEL_DIM), jnp.float32) * MODEL_DIM ** -0.5
    w_o = jax.random.normal(key_list[7], (LAYERS, MODEL_DIM, HEADS * HEAD_DIM), jnp.float32) * (HEADS * HEAD_DIM) ** -0.5
    mlp_gain = jax.random.uniform(key_list[8], (LAYERS, MODEL_DIM), jnp.float32, 0.5, 1.5)
    w_gate_up = jax.random.normal(key_list[9], (LAYERS, 2 * FFN_DIM, MODEL_DIM), jnp.float32) * MODEL_DIM ** -0.5
    w_down = jax.random.normal(key_list[10], (LAYERS, MODEL_DIM, FFN_DIM), jnp.float32) * FFN_DIM ** -0.5
    return {
        "hidden_in": hidden_in.astype(jnp.bfloat16),
        "seq_lens": seq_lens,
        "k_cache": k_cache.astype(jnp.bfloat16),
        "v_cache": v_cache.astype(jnp.bfloat16),
        "attn_gain": attn_gain.astype(jnp.bfloat16),
        "w_qkv": w_qkv.astype(jnp.bfloat16),
        "w_o": w_o.astype(jnp.bfloat16),
        "mlp_gain": mlp_gain.astype(jnp.bfloat16),
        "w_gate_up": w_gate_up.astype(jnp.bfloat16),
        "w_down": w_down.astype(jnp.bfloat16),
    }


def rms_norm(hidden, gain_vec):
    hidden_f32 = hidden.astype(jnp.float32)
    inv_rms = lax.rsqrt(jnp.mean(hidden_f32 * hidden_f32, axis=-1, keepdims=True) + NORM_EPS)
    return (hidden_f32 * inv_rms * gain_vec.astype(jnp.float32)).astype(jnp.bfloat16)


def apply_rope(values, cos_t, sin_t):
    half_dim = values.shape[-1] // 2
    first_half = values[..., :half_dim]
    second_half = values[..., half_dim:]
    return jnp.concatenate([first_half * cos_t - second_half * sin_t, second_half * cos_t + first_half * sin_t], axis=-1)


def reference(hidden_in, seq_lens, k_cache, v_cache, attn_gain, w_qkv, w_o, mlp_gain, w_gate_up, w_down):
    group_rep = HEADS // KV_HEADS
    blocks = w_qkv.reshape(LAYERS, KV_HEADS, group_rep + 2, HEAD_DIM, MODEL_DIM)
    w_query = blocks[:, :, :group_rep].reshape(LAYERS, HEADS * HEAD_DIM, MODEL_DIM)
    w_key = blocks[:, :, group_rep].reshape(LAYERS, KV_HEADS * HEAD_DIM, MODEL_DIM)
    w_value = blocks[:, :, group_rep + 1].reshape(LAYERS, KV_HEADS * HEAD_DIM, MODEL_DIM)
    gen_qkv = jnp.concatenate([
        w_query.reshape(LAYERS, GEN_TP, -1, MODEL_DIM),
        w_key.reshape(LAYERS, GEN_TP, -1, MODEL_DIM),
        w_value.reshape(LAYERS, GEN_TP, -1, MODEL_DIM)], axis=2).reshape(LAYERS, -1, MODEL_DIM)
    fused_rows = w_gate_up.reshape(LAYERS, TRAIN_TP, 2, FFN_DIM // TRAIN_TP, MODEL_DIM)
    w_gate = fused_rows[:, :, 0].reshape(LAYERS, FFN_DIM, MODEL_DIM)
    w_up = fused_rows[:, :, 1].reshape(LAYERS, FFN_DIM, MODEL_DIM)
    gen_gate_up = jnp.stack([
        w_gate.reshape(LAYERS, GEN_TP, -1, MODEL_DIM),
        w_up.reshape(LAYERS, GEN_TP, -1, MODEL_DIM)], axis=2).reshape(LAYERS, 2 * FFN_DIM, MODEL_DIM)

    positions = jnp.arange(CACHE_LEN)
    row_ids = jnp.arange(BATCH)
    inv_freq = jnp.power(ROPE_THETA, -jnp.arange(0, HEAD_DIM, 2).astype(jnp.float32) / HEAD_DIM)
    angles = seq_lens.astype(jnp.float32)[:, None] * inv_freq[None, :]
    cos_t = jnp.cos(angles)[:, None, :]
    sin_t = jnp.sin(angles)[:, None, :]
    score_scale = HEAD_DIM ** -0.5

    def attend_row(row_args):
        query_row, k_row, v_row, length = row_args
        query_grp = query_row.reshape(KV_HEADS, group_rep, HEAD_DIM).astype(jnp.float32)
        scores = jnp.einsum("grd,sgd->grs", query_grp, k_row.astype(jnp.float32)) * score_scale
        scores = jnp.where(positions[None, None, :] <= length, scores, MASK_FILL)
        attn_probs = jax.nn.softmax(scores, axis=-1).astype(jnp.bfloat16)
        out_row = jnp.einsum("grs,sgd->grd", attn_probs.astype(jnp.float32), v_row.astype(jnp.float32))
        return out_row.astype(jnp.bfloat16).reshape(HEADS * HEAD_DIM)

    def layer_step(hidden, layer_xs):
        gain_attn, wgt_query, wgt_key, wgt_value, wgt_out, gain_mlp, wgt_gate, wgt_up, wgt_down, k_layer, v_layer = layer_xs
        normed = rms_norm(hidden, gain_attn)
        query_vals = jnp.dot(normed, wgt_query.T, preferred_element_type=jnp.float32).reshape(BATCH, HEADS, HEAD_DIM)
        key_new = jnp.dot(normed, wgt_key.T, preferred_element_type=jnp.float32).reshape(BATCH, KV_HEADS, HEAD_DIM)
        value_new = jnp.dot(normed, wgt_value.T, preferred_element_type=jnp.float32).reshape(BATCH, KV_HEADS, HEAD_DIM).astype(jnp.bfloat16)
        query_vals = apply_rope(query_vals, cos_t, sin_t).astype(jnp.bfloat16)
        key_new = apply_rope(key_new, cos_t, sin_t).astype(jnp.bfloat16)
        k_layer = k_layer.at[row_ids, seq_lens].set(key_new)
        v_layer = v_layer.at[row_ids, seq_lens].set(value_new)
        attn_out = lax.map(attend_row, (query_vals, k_layer, v_layer, seq_lens))
        attn_proj = jnp.dot(attn_out, wgt_out.T, preferred_element_type=jnp.float32)
        hidden = (hidden.astype(jnp.float32) + attn_proj).astype(jnp.bfloat16)
        normed = rms_norm(hidden, gain_mlp)
        gate_vals = jnp.dot(normed, wgt_gate.T, preferred_element_type=jnp.float32)
        up_vals = jnp.dot(normed, wgt_up.T, preferred_element_type=jnp.float32)
        act_vals = (jax.nn.silu(gate_vals) * up_vals).astype(jnp.bfloat16)
        down_vals = jnp.dot(act_vals, wgt_down.T, preferred_element_type=jnp.float32)
        hidden = (hidden.astype(jnp.float32) + down_vals).astype(jnp.bfloat16)
        return hidden, (k_layer, v_layer)

    layer_xs = (attn_gain, w_query, w_key, w_value, w_o, mlp_gain, w_gate, w_up, w_down, k_cache, v_cache)
    hidden_out, cache_pair = lax.scan(layer_step, hidden_in, layer_xs)
    return (hidden_out, cache_pair[0], cache_pair[1], gen_qkv, gen_gate_up)
```

```python
import functools
import math

import jax
import jax.numpy as jnp
from jax import lax
from jax.experimental import pallas as pl
from jax.experimental.pallas import tpu as pltpu
from jax.sharding import PartitionSpec as P


ROPE_THETA = 500000.0
NORM_EPS = 1e-5
MASK_FILL = -1e30
ROW_AXES = ("pp", "grp")
TRAIN_AXES = ("tg", "grp")
SWAP = [(0, 1), (1, 0)]
ROWS_PER_STEP = 4


def rms_norm(hidden, gain_vec):
    hidden_f32 = hidden.astype(jnp.float32)
    inv_rms = lax.rsqrt(jnp.mean(hidden_f32 * hidden_f32, axis=-1, keepdims=True) + NORM_EPS)
    return (hidden_f32 * inv_rms * gain_vec.astype(jnp.float32)).astype(jnp.bfloat16)


def apply_rope(values, cos_t, sin_t):
    half_dim = values.shape[-1] // 2
    first_half = values[..., :half_dim]
    second_half = values[..., half_dim:]
    return jnp.concatenate([first_half * cos_t - second_half * sin_t, second_half * cos_t + first_half * sin_t], axis=-1)


def rope_tables(lens_f32, head_dim):
    inv_freq = jnp.power(ROPE_THETA, -jnp.arange(0, head_dim, 2).astype(jnp.float32) / head_dim)
    angles = lens_f32[:, None] * inv_freq[None, :]
    return jnp.cos(angles), jnp.sin(angles)


def mm(lhs, rhs):
    return lax.dot_general(lhs, rhs, (((1,), (1,)), ((), ())), preferred_element_type=jnp.float32)


def after(value, *deps):
    return lax.optimization_barrier((value, *deps))[0]


def attn_kernel(heads, seq_ref, q_ref, kn_ref, vn_ref, k_ref, v_ref, *rest):
    ko_ref, vo_ref, o_ref = rest[-3:]
    step = pl.program_id(0)
    rows, flat, head_dim = k_ref.shape[1:]
    lane = lax.broadcasted_iota(jnp.int32, (heads, flat), 1)
    sub = lax.broadcasted_iota(jnp.int32, (heads, flat), 0)
    same_head = (lane % heads) == sub
    pos = lane // heads
    for r in range(rows):
        n = seq_ref[step * rows + r]
        at = pl.ds(pl.multiple_of(n * heads, heads), heads)
        ko_ref[0, r] = k_ref[0, r]
        ko_ref[0, r, at, :] = kn_ref[r]
        vo_ref[0, r] = v_ref[0, r]
        vo_ref[0, r, at, :] = vn_ref[r]
        scores = mm(q_ref[r], ko_ref[0, r]) * head_dim ** -0.5
        scores = jnp.where(same_head & (pos <= n), scores, MASK_FILL)
        top = jnp.max(scores, axis=-1, keepdims=True)
        expd = jnp.exp(scores - top)
        probs = (expd / jnp.sum(expd, axis=-1, keepdims=True)).astype(jnp.bfloat16)
        out = lax.dot_general(probs, vo_ref[0, r], (((1,), (0,)), ((), ())), preferred_element_type=jnp.float32)
        o_ref[r] = out.astype(jnp.bfloat16)


def attend(layer, lens, q, k_new, v_new, k_cache, v_cache, prev):
    _, rows, flat, head_dim = k_cache.shape
    heads = q.shape[1]
    block = ROWS_PER_STEP
    small = pl.BlockSpec((block, heads, head_dim), lambda i, s: (i, 0, 0))
    cache = pl.BlockSpec((1, block, flat, head_dim), lambda i, s: (layer, i, 0, 0))
    hbm = pl.BlockSpec(memory_space=pl.ANY)
    extra = () if prev is None else tuple(prev)
    return pl.pallas_call(
        functools.partial(attn_kernel, heads),
        grid_spec=pltpu.PrefetchScalarGridSpec(
            num_scalar_prefetch=1,
            grid=(rows // block,),
            in_specs=[small, small, small, cache, cache] + [hbm] * len(extra),
            out_specs=[cache, cache, small],
        ),
        out_shape=[jax.ShapeDtypeStruct(k_cache.shape, k_cache.dtype)] * 2
        + [jax.ShapeDtypeStruct(q.shape, jnp.bfloat16)],
        input_output_aliases={} if prev is None else {6: 0, 7: 1},
        cost_estimate=pl.CostEstimate(
            flops=2 * 2 * rows * flat * head_dim * heads,
            bytes_accessed=4 * rows * flat * head_dim * 2, transcendentals=rows * heads * flat),
    )(lens, q, k_new, v_new, k_cache, v_cache, *extra)


def place_kernel(pick, where_ref, first_ref, second_ref, *rest):
    out_ref = rest[-1]
    second = pick(where_ref) != 0

    @pl.when(jnp.logical_not(second))
    def _():
        out_ref[...] = first_ref[...].reshape(out_ref.shape)

    @pl.when(second)
    def _():
        out_ref[...] = second_ref[...].reshape(out_ref.shape)


def place(where, out, first, second, pick, in_block, grid, in_map, out_block, out_map, shape):
    def first_map(i, s):
        return tuple(jnp.where(pick(s) == 0, v, 0) for v in in_map(i))

    def second_map(i, s):
        return tuple(jnp.where(pick(s) == 0, 0, v) for v in in_map(i))

    extra = () if out is None else (out,)
    return pl.pallas_call(
        functools.partial(place_kernel, pick),
        grid_spec=pltpu.PrefetchScalarGridSpec(
            num_scalar_prefetch=1,
            grid=(grid,),
            in_specs=[pl.BlockSpec(in_block, first_map), pl.BlockSpec(in_block, second_map)]
            + [pl.BlockSpec(memory_space=pl.ANY)] * len(extra),
            out_specs=pl.BlockSpec(out_block, out_map),
        ),
        out_shape=jax.ShapeDtypeStruct(shape, first.dtype),
        input_output_aliases={} if out is None else {3: 0},
        cost_estimate=pl.CostEstimate(flops=2 * first.size, bytes_accessed=4 * first.size, transcendentals=0),
    )(where, first, second, *extra)


def solution(mesh):
    cache_spec = P(None, ROW_AXES, None, "tg", None)
    in_specs = (P(ROW_AXES, None), P(ROW_AXES), cache_spec, cache_spec,
                P("pp", None), P("pp", TRAIN_AXES, None), P("pp", None, TRAIN_AXES),
                P("pp", None), P("pp", TRAIN_AXES, None), P("pp", None, TRAIN_AXES))
    out_specs = (P(ROW_AXES, None), cache_spec, cache_spec, P(None, "tg", None), P(None, "tg", None))

    def program(hidden_in, seq_lens, k_cache, v_cache, attn_gain, w_qkv, w_o, mlp_gain, w_gate_up, w_down):
        t, p, g = lax.axis_index("tg"), lax.axis_index("pp"), lax.axis_index("grp")
        rows, dim = hidden_in.shape
        layers, _, cache_len, heads, head_dim = k_cache.shape
        half = dim // 2
        quarter = heads // 2
        ffn = w_gate_up.shape[1] // 2

        wq, wg, wo, wd = w_qkv[0], w_gate_up[0], w_o[0], w_down[0]

        def bulk(value):
            return lax.ppermute(value, ROW_AXES, [(1, 3), (3, 1)])

        def core_swap(value):
            return lax.ppermute(value, "grp", SWAP)

        def forward(value):
            return lax.ppermute(value, "grp", [(1, 0)])

        def x_send(value, src):
            dst = 1 - src
            moved = lax.ppermute(value, "grp", [(1, 0)])
            direct = lax.ppermute(value, ROW_AXES, [(2 * src, 2 * dst)])
            routed = lax.ppermute(moved, ROW_AXES, [(2 * src, 2 * dst + 1)])
            return jnp.where(g == 0, direct, routed)

        def y_swap(value):
            return lax.ppermute(value, "tg", SWAP)

        def halves(value):
            lo, hi = value[:, :half], value[:, half:]
            return jnp.where(t == 0, lo, hi), jnp.where(t == 0, hi, lo)

        def join(mine):
            other = y_swap(mine)
            return jnp.concatenate([jnp.where(t == 0, mine, other), jnp.where(t == 0, other, mine)], axis=1)

        def reduce_half(part, resid):
            mine, theirs = halves(part)
            total = mine + y_swap(theirs)
            return (halves(resid)[0].astype(jnp.float32) + total).astype(jnp.bfloat16)

        rem_q = bulk(wq)
        part_q = core_swap(wq)
        rem_pq = bulk(part_q)

        q_view = (layers, 3, 2, quarter, head_dim, dim)
        g_view = (layers, 2, 2, ffn, dim)
        where = jnp.stack([p, g]).astype(jnp.int32)

        def never(s):
            return 0

        def on_core(s):
            return s[1]

        def own_slot(s):
            return s[0]

        def other_slot(s):
            return 1 - s[0]

        def place_q(out, first, second, pick, slot, src):
            return place(where, out, first.reshape(quarter, 3, head_dim, dim),
                         second.reshape(quarter, 3, head_dim, dim), pick,
                         (quarter, 1, head_dim, dim), 3, lambda i: (0, i, 0, 0),
                         (1, 1, 1, quarter, head_dim, dim), lambda i, s: (slot(s), i, src(s), 0, 0, 0), q_view)

        def place_g(out, first, second, pick, slot, src, start):
            count = first.shape[0]
            base = start % ffn
            unit = ffn // 4 if count % ffn == 0 else math.gcd(count // 2, base)
            per, base = pl.cdiv(ffn, unit), base // unit
            kind = start // ffn
            return place(where, out, first, second, pick, (unit, dim), count // unit, lambda i: (i, 0),
                         (1, 1, 1, unit, dim),
                         lambda i, s: (slot(s), kind + i // per, src(s), base + i % per, 0), g_view)

        gen_q = place_q(None, wq, wq, never, own_slot, lambda s: s[1])
        gen_q = place_q(gen_q, part_q, part_q, never, own_slot, lambda s: 1 - s[1])
        part_g = core_swap(wg)
        gen_g = place_g(None, wg, wg, never, own_slot, lambda s: s[1], 0)
        gen_g = place_g(gen_g, part_g, part_g, never, own_slot, lambda s: 1 - s[1], 0)

        lens_col = jnp.broadcast_to(seq_lens.astype(jnp.bfloat16)[:, None], (rows, 128))
        packed = jnp.concatenate([hidden_in, jnp.broadcast_to(attn_gain, (16, dim))], axis=0)
        packed = x_send(jnp.concatenate([packed, jnp.pad(lens_col, ((0, 16), (0, 0)))], axis=1), 1)
        other_gain = packed[rows, :dim]
        hidden = jnp.concatenate([hidden_in, packed[:rows, :dim]], axis=0)
        lens_f32 = jnp.concatenate([seq_lens.astype(jnp.float32), packed[:rows, dim].astype(jnp.float32)])
        cos_t, sin_t = rope_tables(lens_f32, head_dim)

        part_o = core_swap(wo)
        part_d = core_swap(wd)

        normed = rms_norm(hidden, attn_gain[0])
        own = mm(normed, wq).reshape(2 * rows, quarter, 3, head_dim)
        oth = mm(normed, part_q).reshape(2 * rows, quarter, 3, head_dim)
        proj = jnp.concatenate([jnp.where(g == 0, own, oth), jnp.where(g == 0, oth, own)], axis=1)
        q0 = apply_rope(proj[:, :, 0], cos_t[:, None, :], sin_t[:, None, :])
        k0 = apply_rope(proj[:, :, 1], cos_t[:, None, :], sin_t[:, None, :])
        qkv0 = jnp.concatenate([q0, k0, proj[:, :, 2]], axis=1).astype(jnp.bfloat16)
        qkv0 = qkv0.reshape(2 * rows, 3 * heads * head_dim)
        rem_g = bulk(wg)
        sent = x_send(qkv0[rows:], 0)
        qkv0 = jnp.where(p == 0, qkv0[:rows], sent).reshape(rows, 3, heads, head_dim)

        flat_shape = (layers, rows, cache_len * heads, head_dim)
        k_flat, v_flat = k_cache.reshape(flat_shape), v_cache.reshape(flat_shape)
        k_out, v_out, attn = attend(0, seq_lens, qkv0[:, 0], qkv0[:, 1], qkv0[:, 2], k_flat, v_flat, None)

        cuts = [0, ffn, ffn + 704, ffn + 1056, ffn + 1248, 2 * ffn]
        rem_pg = [bulk(part_g[a:b]) for a, b in zip(cuts[:-1], cuts[1:])]

        def dense_tail(attn_rows, resid):
            lo, hi = attn_rows[:, :quarter * head_dim], attn_rows[:, quarter * head_dim:]
            part = mm(jnp.where(g == 0, lo, hi), wo) + mm(jnp.where(g == 0, hi, lo), part_o)
            mid = join(reduce_half(part, resid))
            a = rms_norm(mid, mlp_gain[0])
            gu, pgu = mm(a, wg), mm(a, part_g)
            act = (jax.nn.silu(gu[:, :ffn]) * gu[:, ffn:]).astype(jnp.bfloat16)
            pact = (jax.nn.silu(pgu[:, :ffn]) * pgu[:, ffn:]).astype(jnp.bfloat16)
            part = mm(act, wd) + mm(pact, part_d)
            return reduce_half(part, mid)

        attn = attn.reshape(rows, heads * head_dim)
        attn_rows = jnp.concatenate([attn, x_send(attn, 1)], axis=0)
        h_half = dense_tail(attn_rows, hidden)
        h_half = jnp.where(p == 0, h_half, x_send(h_half, 0))
        hidden = join(h_half)

        rem_q, rem_pq = after(rem_q, hidden), after(rem_pq, hidden)
        gen_q = place_q(gen_q, forward(rem_q), rem_q, on_core, other_slot, lambda s: 1)
        gen_q = place_q(gen_q, forward(rem_pq), rem_pq, on_core, other_slot, lambda s: 0)
        gen_qkv = gen_q.reshape(layers, 3 * heads * head_dim, dim)

        mine = jnp.where(p == 0, hidden[:rows], hidden[rows:])
        gain1 = jnp.where(p == 0, other_gain, attn_gain[0])
        normed = rms_norm(mine, gain1)
        proj = mm(normed, gen_qkv[1]).reshape(rows, 3, heads, head_dim)
        cos_m, sin_m = cos_t[:rows], sin_t[:rows]
        q1 = apply_rope(proj[:, 0], cos_m[:, None, :], sin_m[:, None, :]).astype(jnp.bfloat16)
        k1 = apply_rope(proj[:, 1], cos_m[:, None, :], sin_m[:, None, :]).astype(jnp.bfloat16)
        v1 = proj[:, 2].astype(jnp.bfloat16)
        k_out, v_out, attn = attend(1, seq_lens, q1, k1, v1, k_flat, v_flat, (k_out, v_out))
        attn = attn.reshape(rows, heads * head_dim)
        attn_rows = jnp.concatenate([x_send(attn, 0), attn], axis=0)
        h_half = dense_tail(attn_rows, hidden)
        h_half = jnp.where(p == 1, h_half[rows:], x_send(h_half[:rows], 1))
        hidden_out = join(h_half)

        rem_g = after(rem_g, hidden_out)
        gen_g = place_g(gen_g, forward(rem_g), rem_g, on_core, other_slot, lambda s: 1, 0)
        for start, piece in zip(cuts, rem_pg):
            piece = after(piece, hidden_out)
            gen_g = place_g(gen_g, forward(piece), piece, on_core, other_slot,
                            lambda s: 0, start)
        gen_gate_up = gen_g.reshape(layers, 4 * ffn, dim)
        return hidden_out, k_out.reshape(k_cache.shape), v_out.reshape(v_cache.shape), gen_qkv, gen_gate_up

    return jax.shard_map(program, mesh=mesh, in_specs=in_specs, out_specs=out_specs, check_vma=False)
```
